256 devices in a mesh: groups: 4 (over y, x), expert: 32 (over z), seq: 2 (over core).
Axes of the slice: x: 2, y: 2, z: 32, core: 2. Of those that a mesh axis runs over, the one named last changes fastest.
The devices are a block of a 4x8x32 slice.
Arguments:
- query: bfloat16 [128, 128, 1024], P(('groups', 'expert')), parts along dimension 0, may hold values from -160 to 160
- key_cache: bfloat16 [128, 768, 1024], P(('groups', 'expert'), 'seq'), parts along dimension 0, may hold values from -4 to 4
- value_cache: bfloat16 [128, 768, 1024], P(('groups', 'expert'), 'seq'), parts along dimension 0, may hold values from -6 to 6
- key_new: bfloat16 [128, 128, 1024], P(('groups', 'expert')), parts along dimension 0, may hold values from -6 to 6
- value_new: bfloat16 [128, 128, 1024], P(('groups', 'expert')), parts along dimension 0, may hold values from -6 to 6
- resid: bfloat16 [128, 128, 1024], P(('groups', 'expert')), parts along dimension 0, may hold values from -6 to 6
- routing: int32 [128, 128, 1], P(('groups', 'expert')), parts along dimension 0, may hold values from 0 to 31; in each aligned block of 128 rows (0 to 127, 128 to 255, ..., all dimensions but the last counted through in order) at most 12 rows name the same one
- router_prob: float32 [128, 128], P(('groups', 'expert')), parts along dimension 0, may hold values from 0.2 to 1
- out_weight: bfloat16 [1024, 1024], replicated, may hold values from -0.1875 to 0.1875
- ffn_gain: float32 [1024], replicated, may hold values from 0.5 to 2
- w_gate: bfloat16 [32, 1024, 2560], P('expert', None, 'seq'), may hold values from -0.1875 to 0.1875
- w_up: bfloat16 [32, 1024, 2560], P('expert', None, 'seq'), may hold values from -0.1875 to 0.1875
- w_down: bfloat16 [32, 2560, 1024], P('expert', 'seq'), may hold values from -0.125 to 0.125
Outputs:
- layer_out: bfloat16 [128, 128, 1024], P(('groups', 'expert')), parts along dimension 0
The draws below stay inside these ranges and needn't reach their ends.
There are 4 independent parts, one for each index of `groups`. The reference program is written for one: setup_inputs(seed, part) draws one part's arguments, and reference() takes and returns one part's arrays. A program takes and returns all parts, laid end to end along the dimension named above; an argument that names none is the same for every part. Nothing has to cross between parts.
Inputs may be any that keep to these rules, and one draw needn't show every extreme that they name: `routing`: among the 128 tokens of one sequence no expert is named more than 12 times, a bound that some block reaches.
All inputs are finite; a program needn't handle non-finite values.
Results may differ from the reference program's by a relative error of at most 0.014.
Values may be sent and summed in bfloat16 or wider, within the bound.
A program may use at most 64 MiB of HBM per device.

```python
import math
import jax
import jax.numpy as jnp
import numpy as np
from jax import lax

MODEL_WIDTH = 1024
HEADS = 16
HEAD_DIM = 64
FF = 2560
QRY = 128
CTX = 768
BATCH = 32
EXPERTS = 32
CAP = 12


def base_keys(key):
    return jnp.clip(jax.random.normal(jax.random.fold_in(key, 31), (BATCH, CTX, MODEL_WIDTH), jnp.float32), -4.0, 4.0)


def draw_key_cache(key, part):
    keys = base_keys(key)
    return keys.astype(jnp.bfloat16)


def draw_query(key, part):
    queries = 2.5 * jnp.clip(jax.random.normal(jax.random.fold_in(key, 53), (BATCH, QRY, MODEL_WIDTH), jnp.float32), -4.0, 4.0)
    return queries.astype(jnp.bfloat16)


def block_scale(stream_key, shape, pieces, least, largest):
    loudness, own = 1.0, jax.random.fold_in(stream_key, 6)
    for dim, blocks in pieces:
        heights = jnp.exp(jax.random.uniform(jax.random.fold_in(own, dim), (blocks,), jnp.float32, least / len(pieces), largest / len(pieces)))
        loudness = loudness * jnp.repeat(heights, shape[dim] // blocks).reshape([-1 if axis == dim else 1 for axis in range(len(shape))])
    return loudness


def shared_out(own_key, own, number, rows, amount, top, reach, slope):
    sequence = jax.random.permutation(own_key, amount)
    packed, usual = load_shares(amount, rows * top, reach, slope, True), load_shares(amount, rows * top, reach, slope, False)
    places = jnp.arange(amount)

    def named(lengths, rotation):
        used = int((lengths > 0).sum())
        fixed = max(1, used // 4)
        passed = fixed + (places - fixed + rotation * (used - fixed)) % max(1, amount - fixed)
        return jnp.zeros((amount,), jnp.int32).at[sequence[jnp.where(places < fixed, places, passed)]].set(jnp.asarray(lengths, jnp.int32))

    lengths = jnp.where(number % 4 == 0, named(packed, number // 4), named(usual, number - number // 4 - 1))
    mixed = jax.random.permutation(jax.random.fold_in(own, 3), amount)
    source_of, taker = mixed[0:amount // 2 * 2:2], mixed[1:amount // 2 * 2:2]
    slack = jnp.minimum(lengths[source_of] - 1, reach - lengths[taker]) // 2
    slack = jnp.where((source_of == sequence[0]) | (taker == sequence[0]) | (lengths[taker] == 0), 0, jnp.maximum(slack, 0))
    passed = jax.random.randint(jax.random.fold_in(own, 4), (amount // 2,), 0, 1 << 20) % (slack + 1)
    lengths = lengths.at[source_of].add(-passed).at[taker].add(passed)
    items = jnp.searchsorted(jnp.cumsum(lengths), jnp.arange(rows * top), side="right").astype(jnp.int32)
    grid = items.reshape(top, rows).T
    grid = grid[jax.random.permutation(jax.random.fold_in(own, 1), rows)]
    rotation = jax.random.randint(jax.random.fold_in(own, 2), (rows, 1), 0, top)
    return jnp.take_along_axis(grid, (jnp.arange(top)[None, :] + rotation) % top, axis=1)


def load_shares(number_of, total, reach, lean, full):
    loads = [(1 << 20) // math.isqrt(grade ** lean) + 1 for grade in range(1, number_of + 1)]
    largest = reach if full else min(reach, max(-(-total // number_of), total * loads[0] // sum(loads)))
    least = 1 if total - largest >= number_of - 1 else 0
    holding, surplus = [largest] + [least] * (number_of - 1), total - largest - least * (number_of - 1)
    while surplus > 0:
        candidates = [i for i in range(1, number_of) if holding[i] < largest] or [i for i in range(1, number_of) if holding[i] < reach]
        pool, left = sum([loads[i] for i in candidates]), surplus
        for i in candidates:
            extra = min(reach - holding[i], max(1, left * loads[i] // pool), surplus)
            holding[i] = holding[i] + extra
            surplus = surplus - extra
    return np.array(holding)


def noise(key, dims, scale, most, split=(), kind=jnp.bfloat16):
    drawn = jax.random.normal(key, dims, jnp.float32) * scale
    if len(split) > 0:
        drawn = block_scale(key, dims, split, -0.22, 0.18) * drawn
    return jnp.clip(drawn, min=-most, max=most).astype(kind)


def setup_inputs(seed: int = 0, part: int = 0) -> dict:
    key_of = jax.random.split(jax.random.key(seed), 14)
    own_keys = jax.random.split(jax.random.fold_in(key_of[13], part), 14)
    query = draw_query(jax.random.fold_in(jax.random.fold_in(key_of[13], part), 71), part)
    key_cache = draw_key_cache(jax.random.fold_in(jax.random.fold_in(key_of[13], part), 71), part)
    value_cache = noise(own_keys[2], (BATCH, CTX, MODEL_WIDTH), 1.0, 6.0, ((0, 32), (1, 2)))
    key_new = noise(own_keys[3], (BATCH, QRY, MODEL_WIDTH), 1.0, 6.0, ((0, 32),))
    value_new = noise(own_keys[4], (BATCH, QRY, MODEL_WIDTH), 1.0, 6.0, ((0, 32),))
    resid = noise(own_keys[5], (BATCH, QRY, MODEL_WIDTH), 1.0, 6.0, ((0, 32),))
    routing_keys = jax.random.split(jax.random.fold_in(own_keys[6], 1), BATCH * QRY // QRY)
    routing_turns = jax.random.permutation(jax.random.fold_in(own_keys[6], 3), BATCH * QRY // QRY)
    routing = jax.vmap(lambda own, number: shared_out(jax.random.fold_in(own_keys[6], 2), own, number, QRY, EXPERTS, 1, CAP, 2))(routing_keys, routing_turns).reshape((BATCH, QRY, 1))
    router_prob = jnp.clip(jnp.exp(math.log(1.0) - 1.609438 * jax.random.uniform(own_keys[7], (BATCH, QRY), jnp.float32) ** block_scale(own_keys[7], (BATCH, QRY), ((0, 32),), -0.2, 0.2)), 0.2, 1.0)
    out_weight = noise(key_of[8], (MODEL_WIDTH, MODEL_WIDTH), MODEL_WIDTH ** -0.5, 0.1875)
    ffn_gain = jnp.clip(jnp.exp(jax.random.uniform(key_of[9], (MODEL_WIDTH,), jnp.float32, math.log(0.5), math.log(2.0))), 0.5, 2.0)
    w_gate = noise(key_of[10], (EXPERTS, MODEL_WIDTH, FF), MODEL_WIDTH ** -0.5, 0.1875, ((0, 32), (2, 2)))
    w_up = noise(key_of[11], (EXPERTS, MODEL_WIDTH, FF), MODEL_WIDTH ** -0.5, 0.1875, ((0, 32), (2, 2)))
    w_down = noise(key_of[12], (EXPERTS, FF, MODEL_WIDTH), FF ** -0.5, 0.125, ((0, 32), (1, 2)))
    return dict(query=query, key_cache=key_cache, value_cache=value_cache, key_new=key_new, value_new=value_new, resid=resid, routing=routing, router_prob=router_prob, out_weight=out_weight, ffn_gain=ffn_gain, w_gate=w_gate, w_up=w_up, w_down=w_down)


def reference(query, key_cache, value_cache, key_new, value_new, resid, routing, router_prob, out_weight, ffn_gain, w_gate, w_up, w_down):
    scale = 1.0 / math.sqrt(HEAD_DIM)
    causal = jnp.arange(QRY)[None, :] <= jnp.arange(QRY)[:, None]
    allowed = jnp.concatenate([jnp.ones((QRY, CTX), dtype=bool), causal], axis=1)

    def attend(inputs):
        queries, keys_old, values_old, candidate_keys, values_fresh = inputs
        heads_q = queries.astype(jnp.float32).reshape(QRY, HEADS, HEAD_DIM)
        keys = jnp.concatenate([keys_old, candidate_keys], axis=0).astype(jnp.float32).reshape(-1, HEADS, HEAD_DIM)
        values = jnp.concatenate([values_old, values_fresh], axis=0).astype(jnp.float32).reshape(-1, HEADS, HEAD_DIM)
        scores = jnp.einsum('qhd,khd->hqk', heads_q, keys) * scale
        scores = jnp.where(allowed[None], scores, -jnp.inf)
        peak = lax.optimization_barrier(jnp.max(scores, axis=2, keepdims=True))
        expw = jnp.exp(scores - peak)
        denom = lax.optimization_barrier(jnp.sum(expw, axis=2))
        weights = lax.optimization_barrier(expw.astype(jnp.bfloat16)).astype(jnp.float32)
        weighted = jnp.einsum('hqk,khd->qhd', weights, values)
        attn = weighted / jnp.transpose(denom)[:, :, None]
        return attn.reshape(QRY, MODEL_WIDTH).astype(jnp.bfloat16)
    attn = lax.map(attend, (query, key_cache, value_cache, key_new, value_new))
    projected = jnp.dot(attn.reshape(-1, MODEL_WIDTH), out_weight, preferred_element_type=jnp.float32).reshape(BATCH, QRY, MODEL_WIDTH)
    hidden = (resid.astype(jnp.float32) + projected).astype(jnp.bfloat16)
    hidden_f = hidden.astype(jnp.float32)
    meansq = lax.optimization_barrier(jnp.mean(hidden_f * hidden_f, axis=-1, keepdims=True))
    normed = (hidden_f * lax.rsqrt(meansq + 1e-06) * ffn_gain.astype(jnp.float32)).astype(jnp.bfloat16)
    normed_features = normed.astype(jnp.float32)
    route = routing[..., 0].astype(jnp.int32)
    onehot = (route[..., None] == jnp.arange(EXPERTS, dtype=jnp.int32)).astype(jnp.int32)
    rank = lax.optimization_barrier(jnp.sum(jnp.cumsum(onehot, axis=1) * onehot, axis=-1)) - 1
    slots = jnp.arange(CAP, dtype=jnp.int32)

    def expert_step(total, item):
        index, gate_w, up_w, down_w = item
        picked = (route == index)[:, None, :] & (rank[:, None, :] == slots[None, :, None])
        expert_selection = picked.astype(jnp.float32)
        token_rows = jnp.einsum('elr,ery->ely', expert_selection, normed_features).astype(jnp.bfloat16).reshape(-1, MODEL_WIDTH)
        gate = jnp.dot(token_rows, gate_w, preferred_element_type=jnp.float32)
        upper = jnp.dot(token_rows, up_w, preferred_element_type=jnp.float32)
        act = (jax.nn.gelu(gate, approximate=True) * upper).astype(jnp.bfloat16)
        expert_result = jnp.dot(act, down_w, preferred_element_type=jnp.float32).astype(jnp.bfloat16)
        expert_result = lax.optimization_barrier(expert_result).astype(jnp.float32).reshape(BATCH, CAP, MODEL_WIDTH)
        returned_output = jnp.einsum('hio,hij->hoj', expert_selection, expert_result)
        return (total + returned_output, None)
    start = jnp.zeros((BATCH, QRY, MODEL_WIDTH), jnp.float32)
    expert_out, unused = lax.scan(expert_step, start, (jnp.arange(EXPERTS, dtype=jnp.int32), w_gate, w_up, w_down))
    return (hidden_f + router_prob.astype(jnp.float32)[..., None] * expert_out).astype(jnp.bfloat16)
```

```python
import functools
import math

import jax
import jax.numpy as jnp
from jax import lax
from jax.experimental import pallas as pl
from jax.experimental.pallas import tpu as pltpu
from jax.sharding import PartitionSpec as P

HEAD_DIM = 64
LANES = 128
GROUP = 8
MESH = pl.DeviceIdType.MESH
NEG = -1e30


def iota(shape, dim):
    return lax.broadcasted_iota(jnp.int32, shape, dim)


def dot(a, b):
    return jnp.dot(a, b, preferred_element_type=jnp.float32)


def dot_t(a, b):
    return lax.dot_general(a, b, (((1,), (1,)), ((), ())), preferred_element_type=jnp.float32)


def attention_kernel(
    query, key_cache, value_cache, key_new, value_new, resid, out_weight, gain,
    hidden_ref, normed_ref,
    q_v, k_v, v_v, r_v, w_v, sums, stats, sums_in, stats_in, attn,
    copy_sem, send_sem, recv_sem,
):
    core = lax.axis_index("seq")
    other = {"seq": 1 - core}
    tokens, width = q_v.shape
    cached = key_cache.shape[0]
    keys = k_v.shape[0]
    pairs = width // LANES
    fresh_half = tokens // 2

    barrier = pltpu.get_barrier_semaphore()
    pl.semaphore_signal(barrier, inc=1, device_id=other, device_id_type=MESH)
    loads = [
        pltpu.make_async_copy(src, dst, copy_sem.at[i])
        for i, (src, dst) in enumerate([
            (query, q_v),
            (key_cache, k_v.at[pl.ds(0, cached)]),
            (key_new, k_v.at[pl.ds(cached, tokens)]),
            (value_cache, v_v.at[pl.ds(0, cached)]),
            (value_new, v_v.at[pl.ds(cached, tokens)]),
            (out_weight, w_v),
            (resid, r_v),
        ])
    ]
    for load in loads:
        load.start()
    stats[...] = jnp.zeros_like(stats)
    pl.semaphore_wait(barrier, 1)
    for load in loads[:5]:
        load.wait()

    def to_other(pair):
        return pltpu.make_async_remote_copy(
            src_ref=sums.at[pair], dst_ref=sums_in.at[pair],
            send_sem=send_sem.at[pair], recv_sem=recv_sem.at[pair],
            device_id=other, device_id_type=MESH,
        )

    low = iota((tokens, LANES), 1) < HEAD_DIM
    lane = iota((tokens, LANES), 1)
    col = iota((2 * tokens, keys), 1) - cached
    row = lax.rem(iota((2 * tokens, keys), 0), tokens)
    mine = lax.div(jnp.maximum(col, 0), fresh_half) == core
    allowed = (col < 0) | ((col <= row) & mine)

    def one_pair(pair, carry):
        lanes = pl.ds(pl.multiple_of(pair * LANES, LANES), LANES)
        q = q_v[:, lanes] * jnp.bfloat16(1.0 / math.sqrt(HEAD_DIM))
        zero = jnp.zeros_like(q)
        both = jnp.concatenate([jnp.where(low, q, zero), jnp.where(low, zero, q)], axis=0)
        scores = jnp.where(allowed, dot_t(both, k_v[:, lanes]), NEG)
        peak = jnp.max(scores, axis=1, keepdims=True)
        expw = jnp.exp(scores - peak)
        denom = jnp.sum(expw, axis=1, keepdims=True)
        weighted = dot(expw.astype(jnp.bfloat16), v_v[:, lanes])
        sums[pair] = jnp.where(low, weighted[:tokens], weighted[tokens:])
        kept = stats[...]
        for side in range(2):
            rows = slice(side * tokens, (side + 1) * tokens)
            head = 2 * pair + side
            kept = jnp.where(lane == head, peak[rows], kept)
            kept = jnp.where(lane == head + 2 * pairs, denom[rows], kept)
        stats[...] = kept
        to_other(pair).start()
        return carry

    lax.fori_loop(0, pairs, one_pair, 0)
    stat_copy = pltpu.make_async_remote_copy(
        src_ref=stats, dst_ref=stats_in, send_sem=send_sem.at[pairs], recv_sem=recv_sem.at[pairs],
        device_id=other, device_id_type=MESH,
    )
    stat_copy.start()
    stat_copy.wait()

    for pair in range(pairs):
        to_other(pair).wait()
        own, their = stats[...], stats_in[...]
        spread = []
        for kind in (own, their):
            for offset in (0, 2 * pairs):
                spots = [kind[:, offset + 2 * pair + side : offset + 2 * pair + side + 1] for side in range(2)]
                spread.append(jnp.where(low, spots[0], spots[1]))
        peak = jnp.maximum(spread[0], spread[2])
        left, right = jnp.exp(spread[0] - peak), jnp.exp(spread[2] - peak)
        denom = spread[1] * left + spread[3] * right
        total = sums[pair] * left + sums_in[pair] * right
        attn[:, pair * LANES : (pair + 1) * LANES] = (total / denom).astype(jnp.bfloat16)

    loads[5].wait()
    loads[6].wait()
    hidden = (r_v[...].astype(jnp.float32) + dot(attn[...], w_v[...])).astype(jnp.bfloat16)
    hidden_ref[...] = hidden
    hidden_f = hidden.astype(jnp.float32)
    meansq = jnp.mean(hidden_f * hidden_f, axis=1, keepdims=True)
    normed_ref[...] = (hidden_f * lax.rsqrt(meansq + 1e-06) * gain[...]).astype(jnp.bfloat16)


def expert_kernel(
    peers, cap,
    normed, hidden, route_col, route_row, prob, w_gate, w_up, w_down,
    out,
    wg, wu, wd, outgoing, arrived, results, returned, total, part, part_in, shuffle, shuffle_t,
    copy_sem, wsend_sem, wrecv_sem, send_sem, recv_sem, back_send, back_recv, last_sem,
):
    me = lax.axis_index("expert")
    core = lax.axis_index("seq")
    other = {"seq": 1 - core}
    tokens, width = normed.shape
    blocks = width // LANES
    slots = cap // 2
    rows = slots * blocks
    group_tokens = GROUP * slots
    group_rows = GROUP * rows
    groups = peers // GROUP
    half = peers // 2
    rels = [half + ((n + 1) // 2) * (1 - 2 * (n % 2)) for n in range(peers)]

    barrier = pltpu.get_barrier_semaphore()
    for rel in rels[:-1]:
        pl.semaphore_signal(barrier, inc=1, device_id={"expert": lax.rem(me + rel, peers)}, device_id_type=MESH)
    pl.semaphore_signal(barrier, inc=1, device_id=other, device_id_type=MESH)
    loads = [
        pltpu.make_async_copy(src, dst.at[0], copy_sem.at[i])
        for i, (src, dst) in enumerate([(w_gate, wg), (w_up, wu), (w_down, wd)])
    ]
    for load in loads:
        load.start()

    same = route_col[...] == route_row[...]
    first, second = iota((tokens, tokens), 0), iota((tokens, tokens), 1)

    def place(route, rank):
        delta = lax.rem(route - me + peers, peers) - half
        order = jnp.where(delta > 0, 2 * delta, jnp.maximum(-2 * delta - 1, 0))
        slot = rank - core * slots
        return jnp.where((slot >= 0) & (slot < slots), order * slots + slot, -1)

    place_col = place(route_col[...], jnp.sum(jnp.where(same & (second < first), 1, 0), axis=1, keepdims=True))
    place_row = place(route_row[...], jnp.sum(jnp.where(same & (first < second), 1, 0), axis=0, keepdims=True))

    def moves(packed, plain):
        peer, block, slot = packed // rows, lax.rem(packed, rows) // slots, lax.rem(packed, slots)
        return jnp.where(plain == block * group_tokens + peer * slots + slot, 1.0, 0.0).astype(jnp.bfloat16)

    square = (group_rows, group_rows)
    shuffle[...] = moves(iota(square, 1), iota(square, 0))
    shuffle_t[...] = moves(iota(square, 0), iota(square, 1))

    def pack(values):
        stacked = jnp.concatenate([values[:, j * LANES : (j + 1) * LANES] for j in range(blocks)], axis=0)
        return dot(shuffle_t[...], stacked).astype(jnp.bfloat16)

    def unpack(packed):
        plain = dot(shuffle[...], packed).astype(jnp.bfloat16)
        return jnp.concatenate(
            [plain[j * group_tokens : (j + 1) * group_tokens] for j in range(blocks)], axis=1
        )

    for g in range(groups):
        picked = jnp.where(
            place_row == g * group_tokens + iota((group_tokens, tokens), 0), 1.0, 0.0
        ).astype(jnp.bfloat16)
        chosen = dot(picked, normed[...]).astype(jnp.bfloat16)
        outgoing[pl.ds(g * group_rows, group_rows)] = pack(chosen)
    own = pl.ds((peers - 1) * rows, rows)
    arrived[own] = outgoing[own]

    pl.semaphore_wait(barrier, peers)
    sends = []
    for n in range(peers - 1):
        spot = pl.ds(n * rows, rows)
        sends.append(pltpu.make_async_remote_copy(
            src_ref=outgoing.at[spot], dst_ref=arrived.at[spot], send_sem=send_sem.at[n], recv_sem=recv_sem.at[n],
            device_id={"expert": lax.rem(me + rels[n], peers)}, device_id_type=MESH,
        ))
        sends[-1].start()
    halves = [
        pltpu.make_async_remote_copy(
            src_ref=src, dst_ref=dst.at[1], send_sem=wsend_sem.at[i], recv_sem=wrecv_sem.at[i],
            device_id=other, device_id_type=MESH,
        )
        for i, (src, dst) in enumerate([(w_gate, wg), (w_up, wu), (w_down, wd)])
    ]
    for copy in halves:
        copy.start()
    for load in loads:
        load.wait()
    for copy in halves:
        copy.wait_recv()

    chunk = 2 * LANES
    chunks = wg.shape[2] // chunk
    backs = []
    for g in range(groups):
        for n in range(g * GROUP, min((g + 1) * GROUP, peers - 1)):
            sends[n].wait_recv()
        rows_in = unpack(arrived[pl.ds(g * group_rows, group_rows)])
        total[...] = jnp.zeros_like(total)

        def step(k, carry, rows_in=rows_in):
            side, at = k // chunks, pl.multiple_of(lax.rem(k, chunks) * chunk, chunk)
            gate = dot(rows_in, wg[side, :, pl.ds(at, chunk)])
            upper = dot(rows_in, wu[side, :, pl.ds(at, chunk)])
            act = (jax.nn.gelu(gate, approximate=True) * upper).astype(jnp.bfloat16)
            total[...] += dot(act, wd[side, pl.ds(at, chunk), :])
            return carry

        lax.fori_loop(0, 2 * chunks, step, 0)
        results[pl.ds(g * group_rows, group_rows)] = pack(total[...].astype(jnp.bfloat16))
        for n in range(g * GROUP, min((g + 1) * GROUP, peers - 1)):
            spot = pl.ds(n * rows, rows)
            backs.append(pltpu.make_async_remote_copy(
                src_ref=results.at[spot], dst_ref=returned.at[spot], send_sem=back_send.at[n], recv_sem=back_recv.at[n],
                device_id={"expert": lax.rem(me + peers - rels[n], peers)}, device_id_type=MESH,
            ))
            backs[-1].start()
    returned[own] = results[own]

    summed = jnp.zeros((tokens, width), jnp.float32)
    for g in range(groups):
        for n in range(g * GROUP, min((g + 1) * GROUP, peers - 1)):
            backs[n].wait_recv()
        rows_back = unpack(returned[pl.ds(g * group_rows, group_rows)])
        picked = jnp.where(
            place_col == g * group_tokens + iota((tokens, group_tokens), 1), 1.0, 0.0
        ).astype(jnp.bfloat16)
        summed += dot(picked, rows_back)
    part[...] = summed.astype(jnp.bfloat16)
    last = pltpu.make_async_remote_copy(
        src_ref=part, dst_ref=part_in, send_sem=last_sem.at[0], recv_sem=last_sem.at[1],
        device_id=other, device_id_type=MESH,
    )
    last.start()
    last.wait_recv()
    expert_out = summed + part_in[...].astype(jnp.float32)
    out[...] = (hidden[...].astype(jnp.float32) + prob[...] * expert_out).astype(jnp.bfloat16)
    for copy in sends + halves + backs + [last]:
        copy.wait_send()


ANY = pl.BlockSpec(memory_space=pl.ANY)
VMEM = pl.BlockSpec(memory_space=pltpu.VMEM)


def on_device(
    peers, query, key_cache, value_cache, key_new, value_new, resid, routing, router_prob,
    out_weight, ffn_gain, w_gate, w_up, w_down,
):
    tokens, width = query.shape[1:]
    cached = key_cache.shape[1]
    keys = cached + tokens
    pairs = width // LANES
    bf16, f32 = jnp.bfloat16, jnp.float32
    hidden, normed = pl.pallas_call(
        attention_kernel,
        name="attention",
        out_shape=[jax.ShapeDtypeStruct((tokens, width), bf16)] * 2,
        in_specs=[ANY] * 7 + [VMEM],
        out_specs=[VMEM, VMEM],
        scratch_shapes=[
            pltpu.VMEM((tokens, width), bf16),
            pltpu.VMEM((keys, width), bf16),
            pltpu.VMEM((keys, width), bf16),
            pltpu.VMEM((tokens, width), bf16),
            pltpu.VMEM(out_weight.shape, bf16),
            pltpu.VMEM((pairs, tokens, LANES), f32),
            pltpu.VMEM((tokens, LANES), f32),
            pltpu.VMEM((pairs, tokens, LANES), f32),
            pltpu.VMEM((tokens, LANES), f32),
            pltpu.VMEM((tokens, width), bf16),
            pltpu.SemaphoreType.DMA((7,)),
            pltpu.SemaphoreType.DMA((pairs + 1,)),
            pltpu.SemaphoreType.DMA((pairs + 1,)),
        ],
        compiler_params=pltpu.CompilerParams(collective_id=1, has_side_effects=True),
    )(
        query[0], key_cache[0], value_cache[0], key_new[0], value_new[0], resid[0],
        out_weight, ffn_gain[None, :],
    )
    cap = max(2, 3 * tokens // peers)
    slots = cap // 2
    total_rows = peers * slots * width // LANES
    group_tokens = GROUP * slots
    group_rows = group_tokens * width // LANES
    hidden_units = w_gate.shape[2]
    route = routing[0]
    result = pl.pallas_call(
        functools.partial(expert_kernel, peers, cap),
        name="experts",
        out_shape=jax.ShapeDtypeStruct((tokens, width), bf16),
        in_specs=[VMEM] * 5 + [ANY] * 3,
        out_specs=VMEM,
        scratch_shapes=[
            pltpu.VMEM((2, width, hidden_units), bf16),
            pltpu.VMEM((2, width, hidden_units), bf16),
            pltpu.VMEM((2, hidden_units, width), bf16),
            pltpu.VMEM((total_rows, LANES), bf16),
            pltpu.VMEM((total_rows, LANES), bf16),
            pltpu.VMEM((total_rows, LANES), bf16),
            pltpu.VMEM((total_rows, LANES), bf16),
            pltpu.VMEM((group_tokens, width), f32),
            pltpu.VMEM((tokens, width), bf16),
            pltpu.VMEM((tokens, width), bf16),
            pltpu.VMEM((group_rows, group_rows), bf16),
            pltpu.VMEM((group_rows, group_rows), bf16),
            pltpu.SemaphoreType.DMA((3,)),
            pltpu.SemaphoreType.DMA((3,)),
            pltpu.SemaphoreType.DMA((3,)),
            pltpu.SemaphoreType.DMA((peers,)),
            pltpu.SemaphoreType.DMA((peers,)),
            pltpu.SemaphoreType.DMA((peers,)),
            pltpu.SemaphoreType.DMA((peers,)),
            pltpu.SemaphoreType.DMA((2,)),
        ],
        compiler_params=pltpu.CompilerParams(
            collective_id=2, has_side_effects=True, vmem_limit_bytes=50 * 1024 * 1024
        ),
    )(
        normed, hidden, route, route.reshape(1, tokens), router_prob.reshape(tokens, 1),
        w_gate[0], w_up[0], w_down[0],
    )
    return result[None]


def solution(mesh):
    in_specs = (
        P(("groups", "expert"), None, None),
        P(("groups", "expert"), "seq", None),
        P(("groups", "expert"), "seq", None),
        P(("groups", "expert"), None, None),
        P(("groups", "expert"), None, None),
        P(("groups", "expert"), None, None),
        P(("groups", "expert"), None, None),
        P(("groups", "expert"), None),
        P(),
        P(),
        P("expert", None, "seq"),
        P("expert", None, "seq"),
        P("expert", "seq", None),
    )
    out_specs = P(("groups", "expert"), None, None)
    return jax.shard_map(
        functools.partial(on_device, mesh.shape["expert"]),
        mesh=mesh, in_specs=in_specs, out_specs=out_specs, check_vma=False,
    )
```

```python
import functools
import math

import jax
import jax.numpy as jnp
from jax import lax
from jax.experimental import pallas as pl
from jax.experimental.pallas import tpu as pltpu
from jax.sharding import PartitionSpec as P

HEAD_DIM = 64
LANES = 128
GROUP = 8
MESH = pl.DeviceIdType.MESH
NEG = -1e30


def iota(shape, dim):
    return lax.broadcasted_iota(jnp.int32, shape, dim)


def dot(a, b):
    return jnp.dot(a, b, preferred_element_type=jnp.float32)


def dot_t(a, b):
    return lax.dot_general(a, b, (((1,), (1,)), ((), ())), preferred_element_type=jnp.float32)


def attention_kernel(
    query, key_cache, value_cache, key_new, value_new,
    attn,
    q_v, k_v, v_v, sums, stats, sums_in, stats_in,
    copy_sem, send_sem, recv_sem,
):
    core = lax.axis_index("seq")
    other = {"seq": 1 - core}
    tokens, width = q_v.shape
    cached = key_cache.shape[0]
    keys = k_v.shape[0]
    pairs = width // LANES
    fresh_half = tokens // 2

    barrier = pltpu.get_barrier_semaphore()
    pl.semaphore_signal(barrier, inc=1, device_id=other, device_id_type=MESH)
    loads = [
        pltpu.make_async_copy(src, dst, copy_sem.at[i])
        for i, (src, dst) in enumerate([
            (query, q_v),
            (key_cache, k_v.at[pl.ds(0, cached)]),
            (key_new, k_v.at[pl.ds(cached, tokens)]),
            (value_cache, v_v.at[pl.ds(0, cached)]),
            (value_new, v_v.at[pl.ds(cached, tokens)]),
        ])
    ]
    for load in loads:
        load.start()
    stats[...] = jnp.zeros_like(stats)
    pl.semaphore_wait(barrier, 1)
    for load in loads:
        load.wait()

    def to_other(pair):
        return pltpu.make_async_remote_copy(
            src_ref=sums.at[pair], dst_ref=sums_in.at[pair],
            send_sem=send_sem.at[pair], recv_sem=recv_sem.at[pair],
            device_id=other, device_id_type=MESH,
        )

    low = iota((tokens, LANES), 1) < HEAD_DIM
    lane = iota((tokens, LANES), 1)
    col = iota((2 * tokens, keys), 1) - cached
    row = lax.rem(iota((2 * tokens, keys), 0), tokens)
    mine = lax.div(jnp.maximum(col, 0), fresh_half) == core
    allowed = (col < 0) | ((col <= row) & mine)

    def one_pair(pair, carry):
        lanes = pl.ds(pl.multiple_of(pair * LANES, LANES), LANES)
        q = q_v[:, lanes] * jnp.bfloat16(1.0 / math.sqrt(HEAD_DIM))
        zero = jnp.zeros_like(q)
        both = jnp.concatenate([jnp.where(low, q, zero), jnp.where(low, zero, q)], axis=0)
        scores = jnp.where(allowed, dot_t(both, k_v[:, lanes]), NEG)
        peak = jnp.max(scores, axis=1, keepdims=True)
        expw = jnp.exp(scores - peak)
        denom = jnp.sum(expw, axis=1, keepdims=True)
        weighted = dot(expw.astype(jnp.bfloat16), v_v[:, lanes])
        sums[pair] = jnp.where(low, weighted[:tokens], weighted[tokens:])
        kept = stats[...]
        for side in range(2):
            rows = slice(side * tokens, (side + 1) * tokens)
            head = 2 * pair + side
            kept = jnp.where(lane == head, peak[rows], kept)
            kept = jnp.where(lane == head + 2 * pairs, denom[rows], kept)
        stats[...] = kept
        to_other(pair).start()
        return carry

    lax.fori_loop(0, pairs, one_pair, 0)
    stat_copy = pltpu.make_async_remote_copy(
        src_ref=stats, dst_ref=stats_in, send_sem=send_sem.at[pairs], recv_sem=recv_sem.at[pairs],
        device_id=other, device_id_type=MESH,
    )
    stat_copy.start()
    stat_copy.wait()

    for pair in range(pairs):
        to_other(pair).wait()
        own, their = stats[...], stats_in[...]
        spread = []
        for kind in (own, their):
            for offset in (0, 2 * pairs):
                spots = [kind[:, offset + 2 * pair + side : offset + 2 * pair + side + 1] for side in range(2)]
                spread.append(jnp.where(low, spots[0], spots[1]))
        peak = jnp.maximum(spread[0], spread[2])
        left, right = jnp.exp(spread[0] - peak), jnp.exp(spread[2] - peak)
        denom = spread[1] * left + spread[3] * right
        total = sums[pair] * left + sums_in[pair] * right
        attn[:, pair * LANES : (pair + 1) * LANES] = (total / denom).astype(jnp.bfloat16)


def expert_kernel(
    peers, cap,
    attn, resid, route_row, prob_row, gain, w_out, w_gate, w_up, w_down,
    out,
    wo, wg, wu, wd, outgoing, arrived, results, returned, total, part, part_in, shuffle, shuffle_t,
    copy_sem, wsend_sem, wrecv_sem, send_sem, recv_sem, back_send, back_recv, last_sem,
):
    me = lax.axis_index("expert")
    core = lax.axis_index("seq")
    other = {"seq": 1 - core}
    tokens, width = attn.shape
    blocks = width // LANES
    slots = cap // 2
    rows = slots * blocks
    group_tokens = GROUP * slots
    group_rows = GROUP * rows
    groups = peers // GROUP
    half = peers // 2

    def ahead(rel):
        return {"expert": lax.rem(me + rel, peers)}

    barrier = pltpu.get_barrier_semaphore()
    pl.semaphore_signal(barrier, inc=1, device_id=other, device_id_type=MESH)
    for rel in range(1, peers):
        pl.semaphore_signal(barrier, inc=1, device_id=ahead(rel), device_id_type=MESH)
    loads = [
        pltpu.make_async_copy(src, dst, copy_sem.at[i])
        for i, (src, dst) in enumerate([
            (w_out, wo), (w_gate, wg.at[0]), (w_up, wu.at[0]), (w_down, wd.at[0]),
        ])
    ]
    for load in loads:
        load.start()

    def place_of(rel):
        if isinstance(rel, int):
            return 2 * (rel - half) if rel > half else max(2 * (half - rel) - 1, 0)
        return jnp.where(rel > half, 2 * (rel - half), jnp.maximum(2 * (half - rel) - 1, 0))

    first, second = iota((tokens, tokens), 0), iota((tokens, tokens), 1)

    def column(row):
        return jnp.sum(jnp.where(first == second, row, jnp.zeros_like(row)), axis=1, keepdims=True)

    route_col = column(route_row[...])
    same = route_col == route_row[...]

    def place(route, rank):
        order = place_of(lax.rem(route - me + peers, peers))
        slot = rank - core * slots
        return jnp.where((slot >= 0) & (slot < slots), order * slots + slot, -1)

    place_col = place(route_col, jnp.sum(jnp.where(same & (second < first), 1, 0), axis=1, keepdims=True))
    place_row = place(route_row[...], jnp.sum(jnp.where(same & (first < second), 1, 0), axis=0, keepdims=True))

    def moves(packed, plain):
        peer, block, slot = packed // rows, lax.rem(packed, rows) // slots, lax.rem(packed, slots)
        return jnp.where(plain == block * group_tokens + peer * slots + slot, 1.0, 0.0).astype(jnp.bfloat16)

    square = (group_rows, group_rows)
    shuffle[...] = moves(iota(square, 1), iota(square, 0))
    shuffle_t[...] = moves(iota(square, 0), iota(square, 1))

    def pack(values):
        stacked = jnp.concatenate([values[:, j * LANES : (j + 1) * LANES] for j in range(blocks)], axis=0)
        return dot(shuffle_t[...], stacked).astype(jnp.bfloat16)

    def unpack(packed):
        plain = dot(shuffle[...], packed).astype(jnp.bfloat16)
        return jnp.concatenate(
            [plain[j * group_tokens : (j + 1) * group_tokens] for j in range(blocks)], axis=1
        )

    loads[0].wait()
    hidden = (resid[...].astype(jnp.float32) + dot(attn[...], wo[...])).astype(jnp.bfloat16)
    hidden_f = hidden.astype(jnp.float32)
    meansq = jnp.mean(hidden_f * hidden_f, axis=1, keepdims=True)
    normed = (hidden_f * lax.rsqrt(meansq + 1e-06) * gain[...]).astype(jnp.bfloat16)

    for g in range(groups):
        picked = jnp.where(
            place_row == g * group_tokens + iota((group_tokens, tokens), 0), 1.0, 0.0
        ).astype(jnp.bfloat16)
        chosen = dot(picked, normed).astype(jnp.bfloat16)
        outgoing[pl.ds(g * group_rows, group_rows)] = pack(chosen)
    own_place = place_of(0)
    own = pl.ds(own_place * rows, rows)
    arrived[own] = outgoing[own]

    def sent(rel):
        n = place_of(rel)
        spot = pl.ds(n * rows, rows)
        return pltpu.make_async_remote_copy(
            src_ref=outgoing.at[spot], dst_ref=arrived.at[spot], send_sem=send_sem.at[n], recv_sem=recv_sem.at[n],
            device_id=ahead(rel), device_id_type=MESH,
        )

    def answered(rel):
        n = place_of(rel)
        spot = pl.ds(n * rows, rows)
        return pltpu.make_async_remote_copy(
            src_ref=results.at[spot], dst_ref=returned.at[spot], send_sem=back_send.at[n], recv_sem=back_recv.at[n],
            device_id=ahead(peers - rel), device_id_type=MESH,
        )

    pl.semaphore_wait(barrier, peers)
    by_place = sorted(range(1, peers), key=place_of)
    for rel in by_place:
        sent(rel).start()
    halves = [
        pltpu.make_async_remote_copy(
            src_ref=src, dst_ref=dst.at[1], send_sem=wsend_sem.at[i], recv_sem=wrecv_sem.at[i],
            device_id=other, device_id_type=MESH,
        )
        for i, (src, dst) in enumerate([(w_gate, wg), (w_up, wu), (w_down, wd)])
    ]
    for copy in halves:
        copy.start()
    for load in loads[1:]:
        load.wait()
    for copy in halves:
        copy.wait_recv()

    members = [[] for _ in range(groups)]
    for rel in by_place:
        members[place_of(rel) // GROUP].append(rel)

    chunk = 2 * LANES
    chunks = wg.shape[2] // chunk
    for g in range(groups):
        for rel in members[g]:
            sent(rel).wait_recv()
        rows_in = unpack(arrived[pl.ds(g * group_rows, group_rows)])
        total[...] = jnp.zeros_like(total)

        def step(k, carry, rows_in=rows_in):
            side, at = k // chunks, pl.multiple_of(lax.rem(k, chunks) * chunk, chunk)
            gate = dot(rows_in, wg[side, :, pl.ds(at, chunk)])
            upper = dot(rows_in, wu[side, :, pl.ds(at, chunk)])
            act = (jax.nn.gelu(gate, approximate=True) * upper).astype(jnp.bfloat16)
            total[...] += dot(act, wd[side, pl.ds(at, chunk), :])
            return carry

        lax.fori_loop(0, 2 * chunks, step, 0)
        results[pl.ds(g * group_rows, group_rows)] = pack(total[...].astype(jnp.bfloat16))
        for rel in members[g]:
            answered(rel).start()
    returned[own] = results[own]

    summed = jnp.zeros((tokens, width), jnp.float32)
    for g in range(groups):
        for rel in members[g]:
            answered(rel).wait_recv()
        rows_back = unpack(returned[pl.ds(g * group_rows, group_rows)])
        picked = jnp.where(
            place_col == g * group_tokens + iota((tokens, group_tokens), 1), 1.0, 0.0
        ).astype(jnp.bfloat16)
        summed += dot(picked, rows_back)
    part[...] = summed.astype(jnp.bfloat16)
    last = pltpu.make_async_remote_copy(
        src_ref=part, dst_ref=part_in, send_sem=last_sem.at[0], recv_sem=last_sem.at[1],
        device_id=other, device_id_type=MESH,
    )
    last.start()
    last.wait_recv()
    expert_out = summed + part_in[...].astype(jnp.float32)
    out[...] = (hidden.astype(jnp.float32) + column(prob_row[...]) * expert_out).astype(jnp.bfloat16)
    for rel in range(1, peers):
        sent(rel).wait_send()
        answered(rel).wait_send()
    for copy in halves + [last]:
        copy.wait_send()


ANY = pl.BlockSpec(memory_space=pl.ANY)
VMEM = pl.BlockSpec(memory_space=pltpu.VMEM)


def on_device(
    peers, query, key_cache, value_cache, key_new, value_new, resid, routing, router_prob,
    out_weight, ffn_gain, w_gate, w_up, w_down,
):
    tokens, width = query.shape[1:]
    cached = key_cache.shape[1]
    keys = cached + tokens
    pairs = width // LANES
    bf16, f32 = jnp.bfloat16, jnp.float32
    attn = pl.pallas_call(
        attention_kernel,
        name="attention",
        out_shape=jax.ShapeDtypeStruct((tokens, width), bf16),
        in_specs=[ANY] * 5,
        out_specs=VMEM,
        scratch_shapes=[
            pltpu.VMEM((tokens, width), bf16),
            pltpu.VMEM((keys, width), bf16),
            pltpu.VMEM((keys, width), bf16),
            pltpu.VMEM((pairs, tokens, LANES), f32),
            pltpu.VMEM((tokens, LANES), f32),
            pltpu.VMEM((pairs, tokens, LANES), f32),
            pltpu.VMEM((tokens, LANES), f32),
            pltpu.SemaphoreType.DMA((5,)),
            pltpu.SemaphoreType.DMA((pairs + 1,)),
            pltpu.SemaphoreType.DMA((pairs + 1,)),
        ],
        compiler_params=pltpu.CompilerParams(collective_id=1, has_side_effects=True),
    )(query[0], key_cache[0], value_cache[0], key_new[0], value_new[0])
    cap = max(2, 3 * tokens // peers)
    slots = cap // 2
    total_rows = peers * slots * width // LANES
    group_tokens = GROUP * slots
    group_rows = group_tokens * width // LANES
    hidden_units = w_gate.shape[2]
    result = pl.pallas_call(
        functools.partial(expert_kernel, peers, cap),
        name="experts",
        out_shape=jax.ShapeDtypeStruct((tokens, width), bf16),
        in_specs=[VMEM] * 5 + [ANY] * 4,
        out_specs=VMEM,
        scratch_shapes=[
            pltpu.VMEM(out_weight.shape, bf16),
            pltpu.VMEM((2, width, hidden_units), bf16),
            pltpu.VMEM((2, width, hidden_units), bf16),
            pltpu.VMEM((2, hidden_units, width), bf16),
            pltpu.VMEM((total_rows, LANES), bf16),
            pltpu.VMEM((total_rows, LANES), bf16),
            pltpu.VMEM((total_rows, LANES), bf16),
            pltpu.VMEM((total_rows, LANES), bf16),
            pltpu.VMEM((group_tokens, width), f32),
            pltpu.VMEM((tokens, width), bf16),
            pltpu.VMEM((tokens, width), bf16),
            pltpu.VMEM((group_rows, group_rows), bf16),
            pltpu.VMEM((group_rows, group_rows), bf16),
            pltpu.SemaphoreType.DMA((4,)),
            pltpu.SemaphoreType.DMA((3,)),
            pltpu.SemaphoreType.DMA((3,)),
            pltpu.SemaphoreType.DMA((peers,)),
            pltpu.SemaphoreType.DMA((peers,)),
            pltpu.SemaphoreType.DMA((peers,)),
            pltpu.SemaphoreType.DMA((peers,)),
            pltpu.SemaphoreType.DMA((2,)),
        ],
        compiler_params=pltpu.CompilerParams(
            collective_id=2, has_side_effects=True, vmem_limit_bytes=50 * 1024 * 1024
        ),
    )(
        attn, resid[0], routing.reshape(1, tokens), router_prob, ffn_gain[None, :],
        out_weight, w_gate[0], w_up[0], w_down[0],
    )
    return result[None]


def solution(mesh):
    in_specs = (
        P(("groups", "expert"), None, None),
        P(("groups", "expert"), "seq", None),
        P(("groups", "expert"), "seq", None),
        P(("groups", "expert"), None, None),
        P(("groups", "expert"), None, None),
        P(("groups", "expert"), None, None),
        P(("groups", "expert"), None, None),
        P(("groups", "expert"), None),
        P(),
        P(),
        P("expert", None, "seq"),
        P("expert", None, "seq"),
        P("expert", "seq", None),
    )
    out_specs = P(("groups", "expert"), None, None)
    return jax.shard_map(
        functools.partial(on_device, mesh.shape["expert"]),
        mesh=mesh, in_specs=in_specs, out_specs=out_specs, check_vma=False,
    )
```

```python
import functools
import math

import jax
import jax.numpy as jnp
from jax import lax
from jax.experimental import pallas as pl
from jax.experimental.pallas import tpu as pltpu
from jax.sharding import PartitionSpec as P

HEAD_DIM = 64
LANES = 128
GROUP = 8
MESH = pl.DeviceIdType.MESH
NEG = -1e30
VMEM_GRANT = 50 * 1024 * 1024


def iota(shape, dim):
    return lax.broadcasted_iota(jnp.int32, shape, dim)


def dot(a, b):
    return jnp.dot(a, b, preferred_element_type=jnp.float32)


def dot_t(a, b):
    return lax.dot_general(a, b, (((1,), (1,)), ((), ())), preferred_element_type=jnp.float32)


def attention_kernel(
    query, key_cache, value_cache, key_new, value_new,
    attn,
    q_v, kc_v, vc_v, kn_v, vn_v, parts, parts_in,
    copy_sem, send_sem, recv_sem,
):
    core = lax.axis_index("seq")
    other = {"seq": 1 - core}
    tokens, width = q_v.shape
    pairs = width // LANES
    fresh_half = tokens // 2
    pieces = 2
    span = width // pieces

    barrier = pltpu.get_barrier_semaphore()
    pl.semaphore_signal(barrier, inc=1, device_id=other, device_id_type=MESH)
    arrays = [(query, q_v), (key_cache, kc_v), (key_new, kn_v), (value_cache, vc_v), (value_new, vn_v)]
    loads = [
        [
            pltpu.make_async_copy(
                src.at[:, pl.ds(piece * span, span)], dst.at[:, pl.ds(piece * span, span)], copy_sem.at[piece, i]
            )
            for i, (src, dst) in enumerate(arrays)
        ]
        for piece in range(pieces)
    ]
    for piece in loads:
        for load in piece:
            load.start()

    def to_other(pair):
        return pltpu.make_async_remote_copy(
            src_ref=parts.at[pair], dst_ref=parts_in.at[pair],
            send_sem=send_sem.at[pair], recv_sem=recv_sem.at[pair],
            device_id=other, device_id_type=MESH,
        )

    low = iota((tokens, LANES), 1) < HEAD_DIM
    col = iota((2 * tokens, tokens), 1)
    row = lax.rem(iota((2 * tokens, tokens), 0), tokens)
    allowed = (col <= row) & (lax.div(col, fresh_half) == core)
    pl.semaphore_wait(barrier, 1)

    def sides(values):
        return jnp.where(low, values[:tokens], values[tokens:])

    def one_pair(pair, carry):
        lanes = pl.ds(pl.multiple_of(pair * LANES, LANES), LANES)
        q = q_v[:, lanes] * jnp.bfloat16(1.0 / math.sqrt(HEAD_DIM))
        zero = jnp.zeros_like(q)
        both = jnp.concatenate([jnp.where(low, q, zero), jnp.where(low, zero, q)], axis=0)
        old = dot_t(both, kc_v[:, lanes])
        new = jnp.where(allowed, dot_t(both, kn_v[:, lanes]), NEG)
        peak = jnp.maximum(jnp.max(old, axis=1, keepdims=True), jnp.max(new, axis=1, keepdims=True))
        exp_old, exp_new = jnp.exp(old - peak), jnp.exp(new - peak)
        denom = jnp.sum(exp_old, axis=1, keepdims=True) + jnp.sum(exp_new, axis=1, keepdims=True)
        weighted = dot(exp_old.astype(jnp.bfloat16), vc_v[:, lanes]) + dot(exp_new.astype(jnp.bfloat16), vn_v[:, lanes])
        spread = (2 * tokens, LANES)
        parts[pair, 0] = sides(weighted)
        parts[pair, 1] = sides(jnp.broadcast_to(peak, spread))
        parts[pair, 2] = sides(jnp.broadcast_to(denom, spread))
        to_other(pair).start()
        return carry

    def merge(pair, carry):
        to_other(pair).wait()
        peak = jnp.maximum(parts[pair, 1], parts_in[pair, 1])
        left, right = jnp.exp(parts[pair, 1] - peak), jnp.exp(parts_in[pair, 1] - peak)
        denom = parts[pair, 2] * left + parts_in[pair, 2] * right
        total = parts[pair, 0] * left + parts_in[pair, 0] * right
        attn[:, pl.ds(pl.multiple_of(pair * LANES, LANES), LANES)] = (total / denom).astype(jnp.bfloat16)
        return carry

    each = pairs // pieces
    for piece in range(pieces):
        for load in loads[piece]:
            load.wait()
        lax.fori_loop(piece * each, (piece + 1) * each, one_pair, 0)
    lax.fori_loop(0, pairs, merge, 0)


def expert_kernel(
    peers, cap,
    attn, resid, route_row, prob_row, gain, w_out, w_gate, w_up, w_down,
    out,
    wg, wu, wd, outgoing, arrived, results, returned, total, part, part_in, shuffle, shuffle_t,
    copy_sem, wsend_sem, wrecv_sem, send_sem, recv_sem, back_send, back_recv, last_sem,
):
    me = lax.axis_index("expert")
    core = lax.axis_index("seq")
    other = {"seq": 1 - core}
    tokens, width = attn.shape
    blocks = width // LANES
    slots = cap // 2
    rows = slots * blocks
    group_tokens = GROUP * slots
    group_rows = GROUP * rows
    groups = peers // GROUP
    half = peers // 2

    def ahead(rel):
        return {"expert": lax.rem(me + rel, peers)}

    barrier = pltpu.get_barrier_semaphore()
    pl.semaphore_signal(barrier, inc=1, device_id=other, device_id_type=MESH)
    for rel in range(1, peers):
        pl.semaphore_signal(barrier, inc=1, device_id=ahead(rel), device_id_type=MESH)
    loads = [
        pltpu.make_async_copy(src, dst, copy_sem.at[i])
        for i, (src, dst) in enumerate([
            (w_gate, wg.at[0]), (w_up, wu.at[0]), (w_down, wd.at[0]),
        ])
    ]
    for load in loads:
        load.start()

    def place_of(rel):
        if isinstance(rel, int):
            return 2 * (rel - half) if rel > half else max(2 * (half - rel) - 1, 0)
        return jnp.where(rel > half, 2 * (rel - half), jnp.maximum(2 * (half - rel) - 1, 0))

    first, second = iota((tokens, tokens), 0), iota((tokens, tokens), 1)

    def column(row):
        return jnp.sum(jnp.where(first == second, row, jnp.zeros_like(row)), axis=1, keepdims=True)

    route_col = column(route_row[...])
    same = route_col == route_row[...]

    def place(route, rank):
        order = place_of(lax.rem(route - me + peers, peers))
        slot = rank - core * slots
        return jnp.where((slot >= 0) & (slot < slots), order * slots + slot, -1)

    place_col = place(route_col, jnp.sum(jnp.where(same & (second < first), 1, 0), axis=1, keepdims=True))
    place_row = place(route_row[...], jnp.sum(jnp.where(same & (first < second), 1, 0), axis=0, keepdims=True))

    def moves(packed, plain):
        peer, block, slot = packed // rows, lax.rem(packed, rows) // slots, lax.rem(packed, slots)
        return jnp.where(plain == block * group_tokens + peer * slots + slot, 1.0, 0.0).astype(jnp.bfloat16)

    square = (group_rows, group_rows)
    shuffle[...] = moves(iota(square, 1), iota(square, 0))
    shuffle_t[...] = moves(iota(square, 0), iota(square, 1))

    def pack(values):
        stacked = jnp.concatenate([values[:, j * LANES : (j + 1) * LANES] for j in range(blocks)], axis=0)
        return dot(shuffle_t[...], stacked).astype(jnp.bfloat16)

    def unpack(packed):
        plain = dot(shuffle[...], packed).astype(jnp.bfloat16)
        return jnp.concatenate(
            [plain[j * group_tokens : (j + 1) * group_tokens] for j in range(blocks)], axis=1
        )

    hidden = (resid[...].astype(jnp.float32) + dot(attn[...], w_out[...])).astype(jnp.bfloat16)
    hidden_f = hidden.astype(jnp.float32)
    meansq = jnp.mean(hidden_f * hidden_f, axis=1, keepdims=True)
    normed = (hidden_f * lax.rsqrt(meansq + 1e-06) * gain[...]).astype(jnp.bfloat16)

    for g in range(groups):
        picked = jnp.where(
            place_row == g * group_tokens + iota((group_tokens, tokens), 0), 1.0, 0.0
        ).astype(jnp.bfloat16)
        chosen = dot(picked, normed).astype(jnp.bfloat16)
        outgoing[pl.ds(g * group_rows, group_rows)] = pack(chosen)
    own_place = place_of(0)
    own = pl.ds(own_place * rows, rows)
    arrived[own] = outgoing[own]

    def sent(rel):
        n = place_of(rel)
        spot = pl.ds(n * rows, rows)
        return pltpu.make_async_remote_copy(
            src_ref=outgoing.at[spot], dst_ref=arrived.at[spot], send_sem=send_sem.at[n], recv_sem=recv_sem.at[n],
            device_id=ahead(rel), device_id_type=MESH,
        )

    def answered(rel):
        n = place_of(rel)
        spot = pl.ds(n * rows, rows)
        return pltpu.make_async_remote_copy(
            src_ref=results.at[spot], dst_ref=returned.at[spot], send_sem=back_send.at[n], recv_sem=back_recv.at[n],
            device_id=ahead(peers - rel), device_id_type=MESH,
        )

    pl.semaphore_wait(barrier, peers)
    by_place = sorted(range(1, peers), key=place_of)
    for rel in by_place:
        sent(rel).start()
    halves = [
        pltpu.make_async_remote_copy(
            src_ref=src, dst_ref=dst.at[1], send_sem=wsend_sem.at[i], recv_sem=wrecv_sem.at[i],
            device_id=other, device_id_type=MESH,
        )
        for i, (src, dst) in enumerate([(w_gate, wg), (w_up, wu), (w_down, wd)])
    ]
    for copy in halves:
        copy.start()
    for load in loads:
        load.wait()
    for copy in halves:
        copy.wait_recv()

    members = [[] for _ in range(groups)]
    for rel in by_place:
        members[place_of(rel) // GROUP].append(rel)

    chunk = 2 * LANES
    chunks = wg.shape[2] // chunk
    for g in range(groups):
        for rel in members[g]:
            sent(rel).wait_recv()
        rows_in = unpack(arrived[pl.ds(g * group_rows, group_rows)])
        total[...] = jnp.zeros_like(total)

        def step(k, carry, rows_in=rows_in):
            side, at = k // chunks, pl.multiple_of(lax.rem(k, chunks) * chunk, chunk)
            gate = dot(rows_in, wg[side, :, pl.ds(at, chunk)])
            upper = dot(rows_in, wu[side, :, pl.ds(at, chunk)])
            act = (jax.nn.gelu(gate, approximate=True) * upper).astype(jnp.bfloat16)
            total[...] += dot(act, wd[side, pl.ds(at, chunk), :])
            return carry

        lax.fori_loop(0, 2 * chunks, step, 0)
        results[pl.ds(g * group_rows, group_rows)] = pack(total[...].astype(jnp.bfloat16))
        for rel in members[g]:
            answered(rel).start()
    returned[own] = results[own]

    summed = jnp.zeros((tokens, width), jnp.float32)
    for g in range(groups):
        for rel in members[g]:
            answered(rel).wait_recv()
        rows_back = unpack(returned[pl.ds(g * group_rows, group_rows)])
        picked = jnp.where(
            place_col == g * group_tokens + iota((tokens, group_tokens), 1), 1.0, 0.0
        ).astype(jnp.bfloat16)
        summed += dot(picked, rows_back)
    part[...] = summed.astype(jnp.bfloat16)
    last = pltpu.make_async_remote_copy(
        src_ref=part, dst_ref=part_in, send_sem=last_sem.at[0], recv_sem=last_sem.at[1],
        device_id=other, device_id_type=MESH,
    )
    last.start()
    last.wait_recv()
    expert_out = summed + part_in[...].astype(jnp.float32)
    out[...] = (hidden.astype(jnp.float32) + column(prob_row[...]) * expert_out).astype(jnp.bfloat16)
    for rel in range(1, peers):
        sent(rel).wait_send()
        answered(rel).wait_send()
    for copy in halves + [last]:
        copy.wait_send()


ANY = pl.BlockSpec(memory_space=pl.ANY)
VMEM = pl.BlockSpec(memory_space=pltpu.VMEM)


def on_device(
    peers, query, key_cache, value_cache, key_new, value_new, resid, routing, router_prob,
    out_weight, ffn_gain, w_gate, w_up, w_down,
):
    tokens, width = query.shape[1:]
    cached = key_cache.shape[1]
    pairs = width // LANES
    bf16, f32 = jnp.bfloat16, jnp.float32
    attn = pl.pallas_call(
        attention_kernel,
        name="attention",
        out_shape=jax.ShapeDtypeStruct((tokens, width), bf16),
        in_specs=[ANY] * 5,
        out_specs=VMEM,
        scratch_shapes=[
            pltpu.VMEM((tokens, width), bf16),
            pltpu.VMEM((cached, width), bf16),
            pltpu.VMEM((cached, width), bf16),
            pltpu.VMEM((tokens, width), bf16),
            pltpu.VMEM((tokens, width), bf16),
            pltpu.VMEM((pairs, 3, tokens, LANES), f32),
            pltpu.VMEM((pairs, 3, tokens, LANES), f32),
            pltpu.SemaphoreType.DMA((2, 5)),
            pltpu.SemaphoreType.DMA((pairs,)),
            pltpu.SemaphoreType.DMA((pairs,)),
        ],
        compiler_params=pltpu.CompilerParams(collective_id=1, has_side_effects=True),
    )(query[0], key_cache[0], value_cache[0], key_new[0], value_new[0])
    cap = max(2, 3 * tokens // peers)
    slots = cap // 2
    total_rows = peers * slots * width // LANES
    group_tokens = GROUP * slots
    group_rows = group_tokens * width // LANES
    hidden_units = w_gate.shape[2]
    result = pl.pallas_call(
        functools.partial(expert_kernel, peers, cap),
        name="experts",
        out_shape=jax.ShapeDtypeStruct((tokens, width), bf16),
        in_specs=[VMEM] * 6 + [ANY] * 3,
        out_specs=VMEM,
        scratch_shapes=[
            pltpu.VMEM((2, width, hidden_units), bf16),
            pltpu.VMEM((2, width, hidden_units), bf16),
            pltpu.VMEM((2, hidden_units, width), bf16),
            pltpu.VMEM((total_rows, LANES), bf16),
            pltpu.VMEM((total_rows, LANES), bf16),
            pltpu.VMEM((total_rows, LANES), bf16),
            pltpu.VMEM((total_rows, LANES), bf16),
            pltpu.VMEM((group_tokens, width), f32),
            pltpu.VMEM((tokens, width), bf16),
            pltpu.VMEM((tokens, width), bf16),
            pltpu.VMEM((group_rows, group_rows), bf16),
            pltpu.VMEM((group_rows, group_rows), bf16),
            pltpu.SemaphoreType.DMA((3,)),
            pltpu.SemaphoreType.DMA((3,)),
            pltpu.SemaphoreType.DMA((3,)),
            pltpu.SemaphoreType.DMA((peers,)),
            pltpu.SemaphoreType.DMA((peers,)),
            pltpu.SemaphoreType.DMA((peers,)),
            pltpu.SemaphoreType.DMA((peers,)),
            pltpu.SemaphoreType.DMA((2,)),
        ],
        compiler_params=pltpu.CompilerParams(
            collective_id=2, has_side_effects=True, vmem_limit_bytes=VMEM_GRANT
        ),
    )(
        attn, resid[0], routing.reshape(1, tokens), router_prob, ffn_gain[None, :],
        out_weight, w_gate[0], w_up[0], w_down[0],
    )
    return result[None]


def solution(mesh):
    in_specs = (
        P(("groups", "expert"), None, None),
        P(("groups", "expert"), "seq", None),
        P(("groups", "expert"), "seq", None),
        P(("groups", "expert"), None, None),
        P(("groups", "expert"), None, None),
        P(("groups", "expert"), None, None),
        P(("groups", "expert"), None, None),
        P(("groups", "expert"), None),
        P(),
        P(),
        P("expert", None, "seq"),
        P("expert", None, "seq"),
        P("expert", "seq", None),
    )
    out_specs = P(("groups", "expert"), None, None)
    return jax.shard_map(
        functools.partial(on_device, mesh.shape["expert"]),
        mesh=mesh, in_specs=in_specs, out_specs=out_specs, check_vma=False,
    )
```

```python
import functools
import math

import jax
import jax.numpy as jnp
from jax import lax
from jax.experimental import pallas as pl
from jax.experimental.pallas import tpu as pltpu
from jax.sharding import PartitionSpec as P

HEAD_DIM = 64
LANES = 128
GROUP = 8
MESH = pl.DeviceIdType.MESH
NEG = -1e30
VMEM_GRANT = 66_600_000


def iota(shape, dim):
    return lax.broadcasted_iota(jnp.int32, shape, dim)


def dot(a, b):
    return jnp.dot(a, b, preferred_element_type=jnp.float32)


def dot_t(a, b):
    return lax.dot_general(a, b, (((1,), (1,)), ((), ())), preferred_element_type=jnp.float32)


def expert_kernel(
    peers, cap,
    query, key_cache, value_cache, key_new, value_new,
    resid_in, route_in, prob_in, gain_in, w_out_in, w_gate, w_up, w_down,
    out,
    resid, route_row, prob_row, gain, w_out, small_sem, q_v, kc_v, vc_v, kn_v, vn_v, parts, parts_in, attn, early_sem, part_send, part_recv,
    wg, wu, wd, outgoing, arrived, results, returned, total, part, part_in, shuffle, shuffle_t,
    copy_sem, wsend_sem, wrecv_sem, send_sem, recv_sem, back_send, back_recv, last_sem,
):
    me = lax.axis_index("expert")
    core = lax.axis_index("seq")
    other = {"seq": 1 - core}
    tokens, width = q_v.shape
    blocks = width // LANES
    slots = cap // 2
    rows = slots * blocks
    group_tokens = GROUP * slots
    group_rows = GROUP * rows
    groups = peers // GROUP
    half = peers // 2

    def ahead(rel):
        return {"expert": lax.rem(me + rel, peers)}

    barrier = pltpu.get_barrier_semaphore()
    pl.semaphore_signal(barrier, inc=1, device_id=other, device_id_type=MESH)
    for rel in range(1, peers):
        pl.semaphore_signal(barrier, inc=1, device_id=ahead(rel), device_id_type=MESH)
    loads = [
        pltpu.make_async_copy(src, dst, copy_sem.at[i])
        for i, (src, dst) in enumerate([
            (w_gate, wg.at[0]), (w_up, wu.at[0]), (w_down, wd.at[0]),
        ])
    ]
    pairs = width // LANES
    fresh_half = tokens // 2
    pieces = 2
    span = width // pieces
    arrays = [(query, q_v), (key_cache, kc_v), (key_new, kn_v), (value_cache, vc_v), (value_new, vn_v)]
    early = [
        [
            pltpu.make_async_copy(
                src.at[:, pl.ds(piece * span, span)], dst.at[:, pl.ds(piece * span, span)], early_sem.at[piece, i]
            )
            for i, (src, dst) in enumerate(arrays)
        ]
        for piece in range(pieces)
    ]
    small = [
        pltpu.make_async_copy(src, dst, small_sem.at[i])
        for i, (src, dst) in enumerate([
            (route_in, route_row), (prob_in, prob_row), (gain_in, gain), (resid_in, resid), (w_out_in, w_out),
        ])
    ]
    for piece in early + [small]:
        for load in piece:
            load.start()

    def to_other(pair):
        return pltpu.make_async_remote_copy(
            src_ref=parts.at[pair], dst_ref=parts_in.at[pair],
            send_sem=part_send.at[pair], recv_sem=part_recv.at[pair],
            device_id=other, device_id_type=MESH,
        )

    low = iota((tokens, LANES), 1) < HEAD_DIM
    col = iota((2 * tokens, tokens), 1)
    row = lax.rem(iota((2 * tokens, tokens), 0), tokens)
    allowed = (col <= row) & (lax.div(col, fresh_half) == core)

    def sides(values):
        return jnp.where(low, values[:tokens], values[tokens:])

    def one_pair(pair, carry):
        lanes = pl.ds(pl.multiple_of(pair * LANES, LANES), LANES)
        q = q_v[:, lanes] * jnp.bfloat16(1.0 / math.sqrt(HEAD_DIM))
        zero = jnp.zeros_like(q)
        both = jnp.concatenate([jnp.where(low, q, zero), jnp.where(low, zero, q)], axis=0)
        old = dot_t(both, kc_v[:, lanes])
        new = jnp.where(allowed, dot_t(both, kn_v[:, lanes]), NEG)
        peak = jnp.maximum(jnp.max(old, axis=1, keepdims=True), jnp.max(new, axis=1, keepdims=True))
        exp_old, exp_new = jnp.exp(old - peak), jnp.exp(new - peak)
        denom = jnp.sum(exp_old, axis=1, keepdims=True) + jnp.sum(exp_new, axis=1, keepdims=True)
        weighted = dot(exp_old.astype(jnp.bfloat16), vc_v[:, lanes]) + dot(exp_new.astype(jnp.bfloat16), vn_v[:, lanes])
        spread = (2 * tokens, LANES)
        parts[pair, 0] = sides(weighted)
        parts[pair, 1] = sides(jnp.broadcast_to(peak, spread))
        parts[pair, 2] = sides(jnp.broadcast_to(denom, spread))
        return carry

    def merge(pair, carry):
        to_other(pair).wait_recv()
        peak = jnp.maximum(parts[pair, 1], parts_in[pair, 1])
        left, right = jnp.exp(parts[pair, 1] - peak), jnp.exp(parts_in[pair, 1] - peak)
        denom = parts[pair, 2] * left + parts_in[pair, 2] * right
        total = parts[pair, 0] * left + parts_in[pair, 0] * right
        attn[:, pl.ds(pl.multiple_of(pair * LANES, LANES), LANES)] = (total / denom).astype(jnp.bfloat16)
        return carry

    each = pairs // pieces
    for piece in range(pieces):
        for load in early[piece]:
            load.wait()
        lax.fori_loop(piece * each, (piece + 1) * each, one_pair, 0)
    for load in loads:
        load.start()
    for load in small:
        load.wait()

    def place_of(rel):
        if isinstance(rel, int):
            return 2 * (rel - half) if rel > half else max(2 * (half - rel) - 1, 0)
        return jnp.where(rel > half, 2 * (rel - half), jnp.maximum(2 * (half - rel) - 1, 0))

    first, second = iota((tokens, tokens), 0), iota((tokens, tokens), 1)

    def column(row):
        return jnp.sum(jnp.where(first == second, row, jnp.zeros_like(row)), axis=1, keepdims=True)

    route_col = column(route_row[...])
    same = route_col == route_row[...]

    def place(route, rank):
        order = place_of(lax.rem(route - me + peers, peers))
        slot = rank - core * slots
        return jnp.where((slot >= 0) & (slot < slots), order * slots + slot, -1)

    place_col = place(route_col, jnp.sum(jnp.where(same & (second < first), 1, 0), axis=1, keepdims=True))
    place_row = place(route_row[...], jnp.sum(jnp.where(same & (first < second), 1, 0), axis=0, keepdims=True))

    def moves(packed, plain):
        peer, block, slot = packed // rows, lax.rem(packed, rows) // slots, lax.rem(packed, slots)
        return jnp.where(plain == block * group_tokens + peer * slots + slot, 1.0, 0.0).astype(jnp.bfloat16)

    square = (group_rows, group_rows)
    shuffle[...] = moves(iota(square, 1), iota(square, 0))
    shuffle_t[...] = moves(iota(square, 0), iota(square, 1))

    def pack(values):
        stacked = jnp.concatenate([values[:, j * LANES : (j + 1) * LANES] for j in range(blocks)], axis=0)
        return dot(shuffle_t[...], stacked).astype(jnp.bfloat16)

    def unpack(packed):
        plain = dot(shuffle[...], packed).astype(jnp.bfloat16)
        return jnp.concatenate(
            [plain[j * group_tokens : (j + 1) * group_tokens] for j in range(blocks)], axis=1
        )

    pl.semaphore_wait(barrier, peers)
    for pair in range(pairs):
        to_other(pair).start()
    lax.fori_loop(0, pairs, merge, 0)
    hidden = (resid[...].astype(jnp.float32) + dot(attn[...], w_out[...])).astype(jnp.bfloat16)
    hidden_f = hidden.astype(jnp.float32)
    meansq = jnp.mean(hidden_f * hidden_f, axis=1, keepdims=True)
    normed = (hidden_f * lax.rsqrt(meansq + 1e-06) * gain[...]).astype(jnp.bfloat16)

    for g in range(groups):
        picked = jnp.where(
            place_row == g * group_tokens + iota((group_tokens, tokens), 0), 1.0, 0.0
        ).astype(jnp.bfloat16)
        chosen = dot(picked, normed).astype(jnp.bfloat16)
        outgoing[pl.ds(g * group_rows, group_rows)] = pack(chosen)
    own_place = place_of(0)
    own = pl.ds(own_place * rows, rows)
    arrived[own] = outgoing[own]

    def sent(rel):
        n = place_of(rel)
        spot = pl.ds(n * rows, rows)
        return pltpu.make_async_remote_copy(
            src_ref=outgoing.at[spot], dst_ref=arrived.at[spot], send_sem=send_sem.at[n], recv_sem=recv_sem.at[n],
            device_id=ahead(rel), device_id_type=MESH,
        )

    def answered(rel):
        n = place_of(rel)
        spot = pl.ds(n * rows, rows)
        return pltpu.make_async_remote_copy(
            src_ref=results.at[spot], dst_ref=returned.at[spot], send_sem=back_send.at[n], recv_sem=back_recv.at[n],
            device_id=ahead(peers - rel), device_id_type=MESH,
        )

    by_place = sorted(range(1, peers), key=place_of)
    for rel in by_place:
        sent(rel).start()
    halves = [
        pltpu.make_async_remote_copy(
            src_ref=src, dst_ref=dst.at[1], send_sem=wsend_sem.at[i], recv_sem=wrecv_sem.at[i],
            device_id=other, device_id_type=MESH,
        )
        for i, (src, dst) in enumerate([(w_gate, wg), (w_up, wu), (w_down, wd)])
    ]
    for copy in halves:
        copy.start()
    for load in loads:
        load.wait()
    for copy in halves:
        copy.wait_recv()

    members = [[] for _ in range(groups)]
    for rel in by_place:
        members[place_of(rel) // GROUP].append(rel)

    chunk = 2 * LANES
    chunks = wg.shape[2] // chunk
    for g in range(groups):
        for rel in members[g]:
            sent(rel).wait_recv()
        rows_in = unpack(arrived[pl.ds(g * group_rows, group_rows)])
        total[...] = jnp.zeros_like(total)

        def step(k, carry, rows_in=rows_in):
            side, at = k // chunks, pl.multiple_of(lax.rem(k, chunks) * chunk, chunk)
            gate = dot(rows_in, wg[side, :, pl.ds(at, chunk)])
            upper = dot(rows_in, wu[side, :, pl.ds(at, chunk)])
            act = (jax.nn.gelu(gate, approximate=True) * upper).astype(jnp.bfloat16)
            total[...] += dot(act, wd[side, pl.ds(at, chunk), :])
            return carry

        lax.fori_loop(0, 2 * chunks, step, 0)
        results[pl.ds(g * group_rows, group_rows)] = pack(total[...].astype(jnp.bfloat16))
        for rel in members[g]:
            answered(rel).start()
    returned[own] = results[own]

    summed = jnp.zeros((tokens, width), jnp.float32)
    for g in range(groups):
        for rel in members[g]:
            answered(rel).wait_recv()
        rows_back = unpack(returned[pl.ds(g * group_rows, group_rows)])
        picked = jnp.where(
            place_col == g * group_tokens + iota((tokens, group_tokens), 1), 1.0, 0.0
        ).astype(jnp.bfloat16)
        summed += dot(picked, rows_back)
    part[...] = summed.astype(jnp.bfloat16)
    last = pltpu.make_async_remote_copy(
        src_ref=part, dst_ref=part_in, send_sem=last_sem.at[0], recv_sem=last_sem.at[1],
        device_id=other, device_id_type=MESH,
    )
    last.start()
    last.wait_recv()
    expert_out = summed + part_in[...].astype(jnp.float32)
    out[...] = (hidden.astype(jnp.float32) + column(prob_row[...]) * expert_out).astype(jnp.bfloat16)
    for rel in range(1, peers):
        sent(rel).wait_send()
        answered(rel).wait_send()
    for copy in halves + [last] + [to_other(pair) for pair in range(pairs)]:
        copy.wait_send()


ANY = pl.BlockSpec(memory_space=pl.ANY)
VMEM = pl.BlockSpec(memory_space=pltpu.VMEM)


def on_device(
    peers, query, key_cache, value_cache, key_new, value_new, resid, routing, router_prob,
    out_weight, ffn_gain, w_gate, w_up, w_down,
):
    tokens, width = query.shape[1:]
    cached = key_cache.shape[1]
    pairs = width // LANES
    bf16, f32 = jnp.bfloat16, jnp.float32
    cap = max(2, 3 * tokens // peers)
    slots = cap // 2
    total_rows = peers * slots * width // LANES
    group_tokens = GROUP * slots
    group_rows = group_tokens * width // LANES
    hidden_units = w_gate.shape[2]
    result = pl.pallas_call(
        functools.partial(expert_kernel, peers, cap),
        name="experts",
        out_shape=jax.ShapeDtypeStruct((tokens, width), bf16),
        in_specs=[ANY] * 13,
        out_specs=VMEM,
        scratch_shapes=[
            pltpu.VMEM((tokens, width), bf16),
            pltpu.VMEM((1, tokens), jnp.int32),
            pltpu.VMEM((1, tokens), f32),
            pltpu.VMEM((1, width), f32),
            pltpu.VMEM(out_weight.shape, bf16),
            pltpu.SemaphoreType.DMA((5,)),
            pltpu.VMEM((tokens, width), bf16),
            pltpu.VMEM((cached, width), bf16),
            pltpu.VMEM((cached, width), bf16),
            pltpu.VMEM((tokens, width), bf16),
            pltpu.VMEM((tokens, width), bf16),
            pltpu.VMEM((pairs, 3, tokens, LANES), f32),
            pltpu.VMEM((pairs, 3, tokens, LANES), f32),
            pltpu.VMEM((tokens, width), bf16),
            pltpu.SemaphoreType.DMA((2, 5)),
            pltpu.SemaphoreType.DMA((pairs,)),
            pltpu.SemaphoreType.DMA((pairs,)),
            pltpu.VMEM((2, width, hidden_units), bf16),
            pltpu.VMEM((2, width, hidden_units), bf16),
            pltpu.VMEM((2, hidden_units, width), bf16),
            pltpu.VMEM((total_rows, LANES), bf16),
            pltpu.VMEM((total_rows, LANES), bf16),
            pltpu.VMEM((total_rows, LANES), bf16),
            pltpu.VMEM((total_rows, LANES), bf16),
            pltpu.VMEM((group_tokens, width), f32),
            pltpu.VMEM((tokens, width), bf16),
            pltpu.VMEM((tokens, width), bf16),
            pltpu.VMEM((group_rows, group_rows), bf16),
            pltpu.VMEM((group_rows, group_rows), bf16),
            pltpu.SemaphoreType.DMA((3,)),
            pltpu.SemaphoreType.DMA((3,)),
            pltpu.SemaphoreType.DMA((3,)),
            pltpu.SemaphoreType.DMA((peers,)),
            pltpu.SemaphoreType.DMA((peers,)),
            pltpu.SemaphoreType.DMA((peers,)),
            pltpu.SemaphoreType.DMA((peers,)),
            pltpu.SemaphoreType.DMA((2,)),
        ],
        compiler_params=pltpu.CompilerParams(
            collective_id=2, has_side_effects=True, vmem_limit_bytes=VMEM_GRANT
        ),
    )(
        query[0], key_cache[0], value_cache[0], key_new[0], value_new[0],
        resid[0], routing.reshape(1, tokens), router_prob, ffn_gain[None, :],
        out_weight, w_gate[0], w_up[0], w_down[0],
    )
    return result[None]


def solution(mesh):
    in_specs = (
        P(("groups", "expert"), None, None),
        P(("groups", "expert"), "seq", None),
        P(("groups", "expert"), "seq", None),
        P(("groups", "expert"), None, None),
        P(("groups", "expert"), None, None),
        P(("groups", "expert"), None, None),
        P(("groups", "expert"), None, None),
        P(("groups", "expert"), None),
        P(),
        P(),
        P("expert", None, "seq"),
        P("expert", None, "seq"),
        P("expert", "seq", None),
    )
    out_specs = P(("groups", "expert"), None, None)
    return jax.shard_map(
        functools.partial(on_device, mesh.shape["expert"]),
        mesh=mesh, in_specs=in_specs, out_specs=out_specs, check_vma=False,
    )
```

```python
import functools
import math

import jax
import jax.numpy as jnp
from jax import lax
from jax.experimental import pallas as pl
from jax.experimental.pallas import tpu as pltpu
from jax.sharding import PartitionSpec as P

HEAD_DIM = 64
LANES = 128
GROUP = 8
MESH = pl.DeviceIdType.MESH
NEG = -1e30
VMEM_GRANT = 66_600_000


def iota(shape, dim):
    return lax.broadcasted_iota(jnp.int32, shape, dim)


def dot(a, b):
    return jnp.dot(a, b, preferred_element_type=jnp.float32)


def dot_t(a, b):
    return lax.dot_general(a, b, (((1,), (1,)), ((), ())), preferred_element_type=jnp.float32)


def expert_kernel(
    peers, cap,
    query, key_cache, value_cache, key_new, value_new,
    resid_in, route_in, prob_in, gain_in, w_out_in, w_gate, w_up, w_down,
    out,
    resid, route_row, prob_row, gain, w_out, small_sem, q_v, kc_v, vc_v, kn_v, vn_v, parts, parts_in, attn, early_sem, part_send, part_recv,
    wg, wu, wd, outgoing, arrived, results, returned, total, part, part_in, shuffle, shuffle_t,
    copy_sem, wsend_sem, wrecv_sem, send_sem, recv_sem, back_send, back_recv, last_sem,
):
    me = lax.axis_index("expert")
    core = lax.axis_index("seq")
    other = {"seq": 1 - core}
    tokens, width = q_v.shape
    blocks = width // LANES
    slots = cap // 2
    rows = slots * blocks
    group_tokens = GROUP * slots
    group_rows = GROUP * rows
    groups = peers // GROUP
    half = peers // 2

    def ahead(rel):
        return {"expert": lax.rem(me + rel, peers)}

    barrier = pltpu.get_barrier_semaphore()
    pl.semaphore_signal(barrier, inc=1, device_id=other, device_id_type=MESH)
    for rel in range(1, peers):
        pl.semaphore_signal(barrier, inc=1, device_id=ahead(rel), device_id_type=MESH)
    loads = [
        pltpu.make_async_copy(src, dst, copy_sem.at[i])
        for i, (src, dst) in enumerate([
            (w_gate, wg.at[0]), (w_up, wu.at[0]), (w_down, wd.at[0]),
        ])
    ]
    pairs = width // LANES
    fresh_half = tokens // 2
    pieces = 2
    span = width // pieces
    arrays = [(query, q_v), (key_cache, kc_v), (key_new, kn_v), (value_cache, vc_v), (value_new, vn_v)]
    early = [
        [
            pltpu.make_async_copy(
                src.at[:, pl.ds(piece * span, span)], dst.at[:, pl.ds(piece * span, span)], early_sem.at[piece, i]
            )
            for i, (src, dst) in enumerate(arrays)
        ]
        for piece in range(pieces)
    ]
    small = [
        pltpu.make_async_copy(src, dst, small_sem.at[i])
        for i, (src, dst) in enumerate([
            (route_in, route_row), (prob_in, prob_row), (gain_in, gain), (resid_in, resid), (w_out_in, w_out),
        ])
    ]
    for piece in early + [small]:
        for load in piece:
            load.start()

    def to_other(pair):
        return pltpu.make_async_remote_copy(
            src_ref=parts.at[pair], dst_ref=parts_in.at[pair],
            send_sem=part_send.at[pair], recv_sem=part_recv.at[pair],
            device_id=other, device_id_type=MESH,
        )

    low = iota((tokens, LANES), 1) < HEAD_DIM
    col = iota((2 * tokens, tokens), 1)
    row = lax.rem(iota((2 * tokens, tokens), 0), tokens)
    allowed = (col <= row) & (lax.div(col, fresh_half) == core)

    def sides(values):
        return jnp.where(low, values[:tokens], values[tokens:])

    def one_pair(pair, carry):
        lanes = pl.ds(pl.multiple_of(pair * LANES, LANES), LANES)
        q = q_v[:, lanes] * jnp.bfloat16(1.0 / math.sqrt(HEAD_DIM))
        zero = jnp.zeros_like(q)
        both = jnp.concatenate([jnp.where(low, q, zero), jnp.where(low, zero, q)], axis=0)
        old = dot_t(both, kc_v[:, lanes])
        new = jnp.where(allowed, dot_t(both, kn_v[:, lanes]), NEG)
        peak = jnp.maximum(jnp.max(old, axis=1, keepdims=True), jnp.max(new, axis=1, keepdims=True))
        exp_old, exp_new = jnp.exp(old - peak), jnp.exp(new - peak)
        denom = jnp.sum(exp_old, axis=1, keepdims=True) + jnp.sum(exp_new, axis=1, keepdims=True)
        weighted = dot(exp_old.astype(jnp.bfloat16), vc_v[:, lanes]) + dot(exp_new.astype(jnp.bfloat16), vn_v[:, lanes])
        spread = (2 * tokens, LANES)
        parts[pair, 0] = sides(weighted)
        parts[pair, 1] = sides(jnp.broadcast_to(peak, spread))
        parts[pair, 2] = sides(jnp.broadcast_to(denom, spread))
        return carry

    def merge(pair, carry):
        to_other(pair).wait_recv()
        peak = jnp.maximum(parts[pair, 1], parts_in[pair, 1])
        left, right = jnp.exp(parts[pair, 1] - peak), jnp.exp(parts_in[pair, 1] - peak)
        denom = parts[pair, 2] * left + parts_in[pair, 2] * right
        total = parts[pair, 0] * left + parts_in[pair, 0] * right
        attn[:, pl.ds(pl.multiple_of(pair * LANES, LANES), LANES)] = (total / denom).astype(jnp.bfloat16)
        return carry

    each = pairs // pieces
    for piece in range(pieces):
        for load in early[piece]:
            load.wait()
        lax.fori_loop(piece * each, (piece + 1) * each, one_pair, 0)
    for load in loads:
        load.start()
    for load in small:
        load.wait()

    def place_of(rel):
        if isinstance(rel, int):
            return 2 * (rel - half) if rel > half else max(2 * (half - rel) - 1, 0)
        return jnp.where(rel > half, 2 * (rel - half), jnp.maximum(2 * (half - rel) - 1, 0))

    first, second = iota((tokens, tokens), 0), iota((tokens, tokens), 1)

    def column(row):
        return jnp.sum(jnp.where(first == second, row, jnp.zeros_like(row)), axis=1, keepdims=True)

    route_col = column(route_row[...])
    same = route_col == route_row[...]

    def place(route, rank):
        order = place_of(lax.rem(route - me + peers, peers))
        slot = rank - core * slots
        return jnp.where((slot >= 0) & (slot < slots), order * slots + slot, -1)

    place_col = place(route_col, jnp.sum(jnp.where(same & (second < first), 1, 0), axis=1, keepdims=True))
    place_row = place(route_row[...], jnp.sum(jnp.where(same & (first < second), 1, 0), axis=0, keepdims=True))

    def moves(packed, plain):
        peer, block, slot = packed // rows, lax.rem(packed, rows) // slots, lax.rem(packed, slots)
        return jnp.where(plain == block * group_tokens + peer * slots + slot, 1.0, 0.0).astype(jnp.bfloat16)

    square = (group_rows, group_rows)
    shuffle[...] = moves(iota(square, 1), iota(square, 0))
    shuffle_t[...] = moves(iota(square, 0), iota(square, 1))

    def pack(values):
        stacked = jnp.concatenate([values[:, j * LANES : (j + 1) * LANES] for j in range(blocks)], axis=0)
        return dot(shuffle_t[...], stacked).astype(jnp.bfloat16)

    def unpack(packed):
        plain = dot(shuffle[...], packed).astype(jnp.bfloat16)
        return jnp.concatenate(
            [plain[j * group_tokens : (j + 1) * group_tokens] for j in range(blocks)], axis=1
        )

    pl.semaphore_wait(barrier, peers)
    for pair in range(pairs):
        to_other(pair).start()
    lax.fori_loop(0, pairs, merge, 0)
    hidden = (resid[...].astype(jnp.float32) + dot(attn[...], w_out[...])).astype(jnp.bfloat16)
    hidden_f = hidden.astype(jnp.float32)
    meansq = jnp.mean(hidden_f * hidden_f, axis=1, keepdims=True)
    normed = (hidden_f * lax.rsqrt(meansq + 1e-06) * gain[...]).astype(jnp.bfloat16)

    def sent(rel):
        n = place_of(rel)
        spot = pl.ds(n * rows, rows)
        return pltpu.make_async_remote_copy(
            src_ref=outgoing.at[spot], dst_ref=arrived.at[spot], send_sem=send_sem.at[n], recv_sem=recv_sem.at[n],
            device_id=ahead(rel), device_id_type=MESH,
        )

    def answered(rel):
        n = place_of(rel)
        spot = pl.ds(n * rows, rows)
        return pltpu.make_async_remote_copy(
            src_ref=results.at[spot], dst_ref=returned.at[spot], send_sem=back_send.at[n], recv_sem=back_recv.at[n],
            device_id=ahead(peers - rel), device_id_type=MESH,
        )

    by_place = sorted(range(1, peers), key=place_of)
    members = [[] for _ in range(groups)]
    for rel in by_place:
        members[place_of(rel) // GROUP].append(rel)
    for g in range(groups):
        picked = jnp.where(
            place_row == g * group_tokens + iota((group_tokens, tokens), 0), 1.0, 0.0
        ).astype(jnp.bfloat16)
        chosen = dot(picked, normed).astype(jnp.bfloat16)
        outgoing[pl.ds(g * group_rows, group_rows)] = pack(chosen)
        for rel in members[g]:
            sent(rel).start()
    own_place = place_of(0)
    own = pl.ds(own_place * rows, rows)
    arrived[own] = outgoing[own]
    halves = [
        pltpu.make_async_remote_copy(
            src_ref=src, dst_ref=dst.at[1], send_sem=wsend_sem.at[i], recv_sem=wrecv_sem.at[i],
            device_id=other, device_id_type=MESH,
        )
        for i, (src, dst) in enumerate([(w_gate, wg), (w_up, wu), (w_down, wd)])
    ]
    for copy in halves:
        copy.start()
    for load in loads:
        load.wait()
    for copy in halves:
        copy.wait_recv()

    chunk = 2 * LANES
    chunks = wg.shape[2] // chunk
    for g in range(groups):
        for rel in members[g]:
            sent(rel).wait_recv()
        rows_in = unpack(arrived[pl.ds(g * group_rows, group_rows)])
        total[...] = jnp.zeros_like(total)

        def step(k, carry, rows_in=rows_in):
            side, at = k // chunks, pl.multiple_of(lax.rem(k, chunks) * chunk, chunk)
            gate = dot(rows_in, wg[side, :, pl.ds(at, chunk)])
            upper = dot(rows_in, wu[side, :, pl.ds(at, chunk)])
            act = (jax.nn.gelu(gate, approximate=True) * upper).astype(jnp.bfloat16)
            total[...] += dot(act, wd[side, pl.ds(at, chunk), :])
            return carry

        lax.fori_loop(0, 2 * chunks, step, 0)
        results[pl.ds(g * group_rows, group_rows)] = pack(total[...].astype(jnp.bfloat16))
        for rel in members[g]:
            answered(rel).start()
    returned[own] = results[own]

    summed = jnp.zeros((tokens, width), jnp.float32)
    for g in range(groups):
        for rel in members[g]:
            answered(rel).wait_recv()
        rows_back = unpack(returned[pl.ds(g * group_rows, group_rows)])
        picked = jnp.where(
            place_col == g * group_tokens + iota((tokens, group_tokens), 1), 1.0, 0.0
        ).astype(jnp.bfloat16)
        summed += dot(picked, rows_back)
    part[...] = summed.astype(jnp.bfloat16)
    last = pltpu.make_async_remote_copy(
        src_ref=part, dst_ref=part_in, send_sem=last_sem.at[0], recv_sem=last_sem.at[1],
        device_id=other, device_id_type=MESH,
    )
    last.start()
    last.wait_recv()
    expert_out = summed + part_in[...].astype(jnp.float32)
    out[...] = (hidden.astype(jnp.float32) + column(prob_row[...]) * expert_out).astype(jnp.bfloat16)
    for rel in range(1, peers):
        sent(rel).wait_send()
        answered(rel).wait_send()
    for copy in halves + [last] + [to_other(pair) for pair in range(pairs)]:
        copy.wait_send()


ANY = pl.BlockSpec(memory_space=pl.ANY)
VMEM = pl.BlockSpec(memory_space=pltpu.VMEM)


def on_device(
    peers, query, key_cache, value_cache, key_new, value_new, resid, routing, router_prob,
    out_weight, ffn_gain, w_gate, w_up, w_down,
):
    tokens, width = query.shape[1:]
    cached = key_cache.shape[1]
    pairs = width // LANES
    bf16, f32 = jnp.bfloat16, jnp.float32
    cap = max(2, 3 * tokens // peers)
    slots = cap // 2
    total_rows = peers * slots * width // LANES
    group_tokens = GROUP * slots
    group_rows = group_tokens * width // LANES
    hidden_units = w_gate.shape[2]
    result = pl.pallas_call(
        functools.partial(expert_kernel, peers, cap),
        name="experts",
        out_shape=jax.ShapeDtypeStruct((tokens, width), bf16),
        in_specs=[ANY] * 13,
        out_specs=VMEM,
        scratch_shapes=[
            pltpu.VMEM((tokens, width), bf16),
            pltpu.VMEM((1, tokens), jnp.int32),
            pltpu.VMEM((1, tokens), f32),
            pltpu.VMEM((1, width), f32),
            pltpu.VMEM(out_weight.shape, bf16),
            pltpu.SemaphoreType.DMA((5,)),
            pltpu.VMEM((tokens, width), bf16),
            pltpu.VMEM((cached, width), bf16),
            pltpu.VMEM((cached, width), bf16),
            pltpu.VMEM((tokens, width), bf16),
            pltpu.VMEM((tokens, width), bf16),
            pltpu.VMEM((pairs, 3, tokens, LANES), f32),
            pltpu.VMEM((pairs, 3, tokens, LANES), f32),
            pltpu.VMEM((tokens, width), bf16),
            pltpu.SemaphoreType.DMA((2, 5)),
            pltpu.SemaphoreType.DMA((pairs,)),
            pltpu.SemaphoreType.DMA((pairs,)),
            pltpu.VMEM((2, width, hidden_units), bf16),
            pltpu.VMEM((2, width, hidden_units), bf16),
            pltpu.VMEM((2, hidden_units, width), bf16),
            pltpu.VMEM((total_rows, LANES), bf16),
            pltpu.VMEM((total_rows, LANES), bf16),
            pltpu.VMEM((total_rows, LANES), bf16),
            pltpu.VMEM((total_rows, LANES), bf16),
            pltpu.VMEM((group_tokens, width), f32),
            pltpu.VMEM((tokens, width), bf16),
            pltpu.VMEM((tokens, width), bf16),
            pltpu.VMEM((group_rows, group_rows), bf16),
            pltpu.VMEM((group_rows, group_rows), bf16),
            pltpu.SemaphoreType.DMA((3,)),
            pltpu.SemaphoreType.DMA((3,)),
            pltpu.SemaphoreType.DMA((3,)),
            pltpu.SemaphoreType.DMA((peers,)),
            pltpu.SemaphoreType.DMA((peers,)),
            pltpu.SemaphoreType.DMA((peers,)),
            pltpu.SemaphoreType.DMA((peers,)),
            pltpu.SemaphoreType.DMA((2,)),
        ],
        compiler_params=pltpu.CompilerParams(
            collective_id=2, has_side_effects=True, vmem_limit_bytes=VMEM_GRANT
        ),
    )(
        query[0], key_cache[0], value_cache[0], key_new[0], value_new[0],
        resid[0], routing.reshape(1, tokens), router_prob, ffn_gain[None, :],
        out_weight, w_gate[0], w_up[0], w_down[0],
    )
    return result[None]


def solution(mesh):
    in_specs = (
        P(("groups", "expert"), None, None),
        P(("groups", "expert"), "seq", None),
        P(("groups", "expert"), "seq", None),
        P(("groups", "expert"), None, None),
        P(("groups", "expert"), None, None),
        P(("groups", "expert"), None, None),
        P(("groups", "expert"), None, None),
        P(("groups", "expert"), None),
        P(),
        P(),
        P("expert", None, "seq"),
        P("expert", None, "seq"),
        P("expert", "seq", None),
    )
    out_specs = P(("groups", "expert"), None, None)
    return jax.shard_map(
        functools.partial(on_device, mesh.shape["expert"]),
        mesh=mesh, in_specs=in_specs, out_specs=out_specs, check_vma=False,
    )
```
